32 devices in a mesh: dp: 8 (over z, x), entry: 4 (over y, core).
Axes of the slice: x: 2, y: 2, z: 4, core: 2. Of those that a mesh axis runs over, the one named last changes fastest.
Arguments:
- frames: float32 [2048, 1024], P('dp'), may hold values from -100 to 100, as said below
- depth: int32 [8], P('dp'), may hold values from 1 to 2
- code_one: float32 [8192, 1024], P(('entry', 'dp')), may hold values from -0.5 to 0.5, as said below
- code_two: float32 [8192, 1024], P(('entry', 'dp')), may hold values from -0.5 to 0.5, as said below
Outputs:
- new_one: float32 [8192, 1024], P(('entry', 'dp'))
- new_two: float32 [8192, 1024], P(('entry', 'dp'))
The draws below stay inside these ranges and needn't reach their ends.
Inputs may be any that keep to these rules, and one draw needn't show every extreme that they name: `frames`: Real-valued embeddings. `code_one`: Real-valued entries. `code_two`: Real-valued entries.
All inputs are finite; a program needn't handle non-finite values.
Results may differ from the reference program's by a relative error of at most 0.012.
Values may be sent and summed in bfloat16 or wider, within the bound.
No kernel may reach another device: no remote copies, remote signals or barrier semaphores. Data moves between devices by JAX's collectives and lax.ppermute only.
A program may use at most 128 MiB of HBM per device.

```python
import jax
import jax.numpy as jnp
from jax import lax

D = 1024
K = 8192
GROUP = 256
GROUPS = 8
FRAMES = 2048


def codebooks(key):
    first_key, second_key, third_key = jax.random.split(jax.random.fold_in(key, 11), 3)
    spread = 4.0 / D ** 0.5
    first = spread * jnp.clip(jax.random.normal(first_key, (K, D), jnp.float32), -4.0, 4.0)
    second = spread * jnp.clip(jax.random.normal(second_key, (K, D), jnp.float32), -4.0, 4.0)
    nudge = 0.0625 / D ** 0.5 * jax.random.normal(third_key, (8, D), jnp.float32)
    evens = first[0:16:2]
    first = first.at[1:16:2].set(jnp.clip(evens + nudge, -4.0 * spread, 4.0 * spread))
    return (first, second)


def draw_code_one(key, part):
    return codebooks(key)[0]


def draw_code_two(key, part):
    return codebooks(key)[1]


def draw_frames(key, part):
    first, second = codebooks(key)
    base_key = jax.random.fold_in(jax.random.fold_in(key, 23), 0)
    values = jnp.clip(jax.random.normal(base_key, (FRAMES, D), jnp.float32), -6.0, 6.0)
    chosen = FRAMES - 8 + jnp.arange(8)
    target = first[0:16:2]
    length = jnp.sum(target * target, axis=1, keepdims=True)
    strength = jnp.linspace(100.0, 250.0, 8).astype(jnp.float32)[:, None]
    planted = strength / length * target + 0.05 * values[chosen]
    values = values.at[chosen].set(planted)
    return values


def plant(result, rng, least, largest):
    longest = result.shape.index(max(result.shape))
    spots = []
    for shift in (0, 1):
        where = [jax.random.randint(jax.random.fold_in(rng, axis), (), 0, length) for axis, length in enumerate(result.shape)]
        where[longest] = (where[longest] + shift) % result.shape[longest]
        spots.append(tuple(where))
    return result.at[spots[0]].set(least).at[spots[1]].set(largest)


def setup_inputs(seed: int = 0) -> dict:
    seeds = jax.random.split(jax.random.key(seed), 5)
    frames = draw_frames(jax.random.fold_in(seeds[4], 71), 0)
    depth = plant(jax.random.randint(seeds[1], (GROUPS,), 1, 3), jax.random.fold_in(seeds[1], 1), 1, 2).astype(jnp.int32)
    code_one = draw_code_one(jax.random.fold_in(seeds[4], 71), 0)
    code_two = draw_code_two(jax.random.fold_in(seeds[4], 71), 0)
    return {"frames": frames, "depth": depth, "code_one": code_one, "code_two": code_two}


def soft_step(code, rows, weight, rebuild):
    book = code.astype(jnp.bfloat16)
    wide = book.astype(jnp.float32)
    half = 0.5 * jnp.sum(wide * wide, axis=1)
    blocks = rows.reshape(GROUPS, GROUP, D)

    def visit(carry, item):
        block, share = item
        narrow = block.astype(jnp.bfloat16)
        score = jnp.dot(narrow, book.T, preferred_element_type=jnp.float32) - half[None, :]
        peak = jnp.max(score, axis=1, keepdims=True)
        expo = jnp.exp(score - peak)
        prob = expo / jnp.sum(expo, axis=1, keepdims=True)
        rounded = prob.astype(jnp.bfloat16)
        masked = rounded * share.astype(jnp.bfloat16)
        num = carry[0] + jnp.dot(masked.T, narrow, preferred_element_type=jnp.float32)
        den = carry[1] + share * jnp.sum(prob, axis=0)
        if rebuild:
            rebuilt = (block - jnp.dot(rounded, book, preferred_element_type=jnp.float32)).astype(jnp.bfloat16)
        else:
            rebuilt = jnp.zeros((GROUP, D), jnp.bfloat16)
        return (num, den), rebuilt

    start = (jnp.zeros((K, D), jnp.float32), jnp.zeros((K,), jnp.float32))
    (num, den), rest = lax.scan(visit, start, (blocks, weight))
    fresh = (num + code) / (den[:, None] + 1.0)
    return fresh, rest.reshape(FRAMES, D)


def reference(frames, depth, code_one, code_two):
    ones = jnp.ones((GROUPS,), jnp.float32)
    new_one, second = soft_step(code_one, frames, ones, True)
    deep = (depth == 2).astype(jnp.float32)
    new_two, unused = soft_step(code_two, second.astype(jnp.float32), deep, False)
    return new_one, new_two
```

```python
import functools
import math

import jax
import jax.numpy as jnp
from jax import lax
from jax.experimental import pallas as pl
from jax.experimental.pallas import tpu as pltpu
from jax.sharding import PartitionSpec as P


EXTRA = 128
FAR = 3.0e38
NT = (((1,), (1,)), ((), ()))
NN = (((1,), (0,)), ((), ()))
BF = jnp.bfloat16
F32 = jnp.float32


def as_row(column):
    return jnp.broadcast_to(column, (column.shape[0], EXTRA)).T[0:1, :]


def half_column(book):
    wide = book.astype(F32)
    return 0.5 * jnp.sum(wide * wide, axis=1, keepdims=True)


def split(value):
    high = value.astype(BF).astype(F32)
    rest = value - high
    middle = rest.astype(BF).astype(F32)
    return high, middle, rest - middle


def attend_kernel(n_rows, n_books, rebuild, *refs):
    row_refs, book_refs = refs[:n_rows], refs[n_rows : n_rows + n_books]
    outs, (rows, score) = refs[n_rows + n_books : -2], refs[-2:]
    part = row_refs[0].shape[0]
    entries = book_refs[0].shape[0]
    for j in range(n_rows):
        rows[j * part : (j + 1) * part, :] = row_refs[j][...]
    peak = None
    for j in range(n_books):
        book = book_refs[j][...]
        s = lax.dot_general(rows[...], book, NT, preferred_element_type=F32)
        s = s - as_row(half_column(book))
        score[j] = s
        top = jnp.max(s, axis=1, keepdims=True)
        peak = top if peak is None else jnp.maximum(peak, top)
    total = None
    rebuilt = None
    for j in range(n_books):
        expo = jnp.exp(score[j] - peak)
        mass = jnp.sum(expo, axis=1, keepdims=True)
        total = mass if total is None else total + mass
        if rebuild:
            term = lax.dot_general(expo.astype(BF), book_refs[j][...], NN, preferred_element_type=F32)
            rebuilt = term if rebuilt is None else rebuilt + term
    level = peak + jnp.log(total)
    if not rebuild:
        outs[0][...] = as_row(level)
        return
    width = rebuilt.shape[1]
    rebuilt = rebuilt / total
    high, middle, low = split(level)
    lane = lax.broadcasted_iota(jnp.int32, (level.shape[0], EXTRA), 1)
    tail = jnp.where(lane == 0, high, jnp.where(lane == 1, middle, jnp.where(lane == 2, low, 0.0)))
    for j in range(n_rows):
        here = slice(j * part, (j + 1) * part)
        outs[j][:, :width] = rebuilt[here].astype(BF)
        outs[j][:, width:] = tail[here].astype(BF)


def attend(rows, books, part, rebuild):
    width = books[0].shape[1]
    entries = books[0].shape[0]
    frames = part * len(rows)
    if rebuild:
        out_shape = [jax.ShapeDtypeStruct((part, width + EXTRA), BF)] * len(rows)
    else:
        out_shape = [jax.ShapeDtypeStruct((1, frames), F32)]
    whole = pl.BlockSpec(memory_space=pltpu.VMEM)
    work = 2 * frames * entries * len(books) * width
    return pl.pallas_call(
        functools.partial(attend_kernel, len(rows), len(books), rebuild),
        grid=(1,),
        out_shape=out_shape,
        in_specs=[pl.BlockSpec((part, width), lambda i: (0, 0))] * len(rows)
        + [pl.BlockSpec((entries, width), lambda i: (0, 0))] * len(books),
        out_specs=[pl.BlockSpec(s.shape, lambda i: (0, 0)) for s in out_shape],
        scratch_shapes=[
            pltpu.VMEM((frames, width), BF),
            pltpu.VMEM((len(books), frames, entries), F32),
        ],
        compiler_params=pltpu.CompilerParams(vmem_limit_bytes=48 * 1024 * 1024),
        cost_estimate=pl.CostEstimate(
            flops=work * (2 if rebuild else 1),
            bytes_accessed=2 * width * (frames + entries * len(books)),
            transcendentals=frames * entries * len(books),
        ),
        name="attend" if rebuild else "levels",
    )(*rows, *books)


def sums_kernel(n_chunks, *refs):
    chunk_refs, (level_ref, book_ref, out_ref) = refs[:n_chunks], refs[n_chunks:]
    book = book_ref[...]
    width = book.shape[1]
    half = half_column(book)
    num = None
    den = None
    for j in range(n_chunks):
        chunk = chunk_refs[j][...]
        s = lax.dot_general(book, chunk, NT, preferred_element_type=F32) - half
        prob = jnp.exp(s - level_ref[j : j + 1, :])
        count = jnp.sum(prob, axis=1, keepdims=True)
        term = lax.dot_general(prob.astype(BF), chunk, NN, preferred_element_type=F32)
        num = term if num is None else num + term
        den = count if den is None else den + count
    out_ref[:, :width] = num
    out_ref[:, width:] = jnp.broadcast_to(den, (den.shape[0], EXTRA))


def sums(chunks, levels, book):
    entries, width = book.shape
    frames = sum(chunk.shape[0] for chunk in chunks)
    return pl.pallas_call(
        functools.partial(sums_kernel, len(chunks)),
        out_shape=jax.ShapeDtypeStruct((entries, width + EXTRA), F32),
        in_specs=[pl.BlockSpec(memory_space=pltpu.VMEM)] * (len(chunks) + 2),
        out_specs=pl.BlockSpec(memory_space=pltpu.VMEM),
        compiler_params=pltpu.CompilerParams(vmem_limit_bytes=48 * 1024 * 1024),
        cost_estimate=pl.CostEstimate(
            flops=4 * frames * entries * width,
            bytes_accessed=2 * width * frames + 6 * width * entries,
            transcendentals=frames * entries,
        ),
        name="sums",
    )(*chunks, levels, book)


def merge_levels(parts):
    top = functools.reduce(jnp.maximum, parts)
    return top + jnp.log(sum(jnp.exp(part - top) for part in parts))


def refresh(mine, received, code):
    width = code.shape[1]
    total = functools.reduce(lambda a, b: a + b, received, mine)
    return (total[:, :width] + code) / (total[:, width : width + 1] + 1.0)


def build(lz, lx, ly, lc):
    entry = ly * lc
    axes = ("dp", "entry")
    sizes = (lz, lx, ly, lc)

    def shift(value, z=0, x=0, y=0, c=0):
        pairs = []
        for source in range(lz * lx * entry):
            rest, place = source, []
            for size in reversed(sizes):
                rest, digit = divmod(rest, size)
                place.append(digit)
            to = 0
            for digit, size, step in zip(reversed(place), sizes, (z, x, y, c)):
                to = to * size + (digit + step) % size
            pairs.append((source, to))
        return lax.ppermute(value, axes, pairs)

    around = [(i, k) for i in range(lx) for k in range(ly)]

    def layer(book, after=None):
        near = [shift(book, c=m) for m in range(1, lc)]
        if after is not None:
            book, _ = lax.optimization_barrier((book, after))
        far = [shift(book, x=i, y=k) for i, k in around[1:]]
        across = [shift(piece, c=m) for piece in far for m in range(1, lc)]
        return [book] + near, far + across

    def on_device(frames, depth, code_one, code_two):
        place = lax.axis_index("entry")
        y, c = place // lc, place % lc
        part = frames.shape[0] // entry
        width = frames.shape[1]
        book_one = code_one.astype(BF)
        book_two = code_two.astype(BF)
        near_one, far_one = layer(book_one)
        starts = [(c * ly + (y - k) % ly) * part for k in range(ly)]
        own = jnp.concatenate([lax.dynamic_slice_in_dim(frames, s, part, 0) for s in starts], 0).astype(BF)
        slabs = [own] + [shift(own, z=j) for j in range(1, lz)]
        pieces = attend(slabs, near_one + far_one, part, True)
        returned = [pieces[0]] + [shift(pieces[j], z=-j) for j in range(1, lz)]
        near_two, far_two = layer(book_two, far_one[len(around) - 2])

        mine = [
            jnp.concatenate([slab[k * part : (k + 1) * part] for slab in slabs], 0) for k in range(ly)
        ]
        chunks_one = list(mine)
        first, _ = lax.optimization_barrier((mine[0], far_one[len(around) - 2]))
        for i in range(1, lx):
            moved = shift(first, x=i)
            chunks_one.append(moved)
            chunks_one.extend(shift(moved, y=k) for k in range(1, ly))

        tails = [piece[:, width : width + 3].astype(F32) for piece in returned]
        parts = [tail[:, 0:1] + tail[:, 1:2] + tail[:, 2:3] for tail in tails]
        level = merge_levels(parts)
        rebuilt = sum(jnp.exp(p - level) * r[:, :width].astype(F32) for p, r in zip(parts, returned))
        second = (lax.dynamic_slice_in_dim(frames, starts[0], part, 0) - rebuilt).astype(BF)
        group = frames.shape[0] // depth.shape[0]
        weight = jnp.repeat((depth == 2).astype(F32), group)
        weight = lax.dynamic_slice_in_dim(weight, starts[0], part, 0)

        seconds = [second] + [shift(second, z=j) for j in range(1, lz)]
        joined = jnp.concatenate(seconds, 0)
        chunks_two = [joined] + [shift(joined, x=i, y=k) for i, k in around[1:]]
        (local,) = attend(seconds, near_two + far_two, part, False)
        note = jnp.concatenate([local, level.reshape(1, part), weight.reshape(1, part)], 1)
        notes = [note] + [shift(note, z=j) for j in range(1, lz)]
        many = lz * part
        level_two = merge_levels(
            [jnp.roll(n[0, :many].reshape(lz, part), j, axis=0) for j, n in enumerate(notes)]
        ).reshape(1, many)
        level_one = jnp.concatenate([n[:, many : many + part] for n in notes], 1)
        weights = jnp.concatenate([n[:, many + part :] for n in notes], 1)
        level_two = jnp.where(weights > 0.0, level_two, FAR)
        stats = jnp.concatenate([level_one, level_two], 0)
        all_stats = [stats] + [shift(stats, x=i, y=k) for i, k in around[1:]]
        levels_one = jnp.concatenate([s[0:1] for s in all_stats], 0)
        levels_two = jnp.concatenate([s[1:2] for s in all_stats], 0)

        sent_one = [shift(sums(chunks_one, levels_one, near_one[m]), c=-m) for m in range(1, lc)]
        sum_one = sums(chunks_one, levels_one, near_one[0])
        sent_two = [shift(sums(chunks_two, levels_two, near_two[m]), c=-m) for m in range(1, lc)]
        sum_two = sums(chunks_two, levels_two, near_two[0])
        return refresh(sum_one, sent_one, code_one), refresh(sum_two, sent_two, code_two)

    return on_device


def solution(mesh):
    dp, entry = mesh.shape["dp"], mesh.shape["entry"]
    lz = math.gcd(dp, entry)
    lc = 2 if entry % 2 == 0 else 1
    return jax.shard_map(
        build(lz, dp // lz, entry // lc, lc),
        mesh=mesh,
        in_specs=(P("dp", None), P("dp"), P(("entry", "dp"), None), P(("entry", "dp"), None)),
        out_specs=(P(("entry", "dp"), None), P(("entry", "dp"), None)),
        check_vma=False,
    )
```

```python
import functools
import math

import jax
import jax.numpy as jnp
from jax import lax
from jax.experimental import pallas as pl
from jax.experimental.pallas import tpu as pltpu
from jax.sharding import PartitionSpec as P


EXTRA = 128
BYTES = 28 * 1024 * 1024
FAR = 3.0e38
NT = (((1,), (1,)), ((), ()))
NN = (((1,), (0,)), ((), ()))
BF = jnp.bfloat16
F32 = jnp.float32


def as_row(column):
    return jnp.broadcast_to(column, (column.shape[0], EXTRA)).T[0:1, :]


def half_column(book):
    wide = book.astype(F32)
    return 0.5 * jnp.sum(wide * wide, axis=1, keepdims=True)


def split(value):
    high = value.astype(BF).astype(F32)
    rest = value - high
    middle = rest.astype(BF).astype(F32)
    return high, middle, rest - middle


def attend_kernel(n_rows, n_books, rebuild, *refs):
    row_refs, book_refs = refs[:n_rows], refs[n_rows : n_rows + n_books]
    outs, (rows, score) = refs[n_rows + n_books : -2], refs[-2:]
    part = row_refs[0].shape[0]
    for j in range(n_rows):
        rows[j * part : (j + 1) * part, :] = row_refs[j][...]
    peak = None
    for j in range(n_books):
        book = book_refs[j][...]
        s = lax.dot_general(rows[...], book, NT, preferred_element_type=F32)
        s = s - as_row(half_column(book))
        score[j, :, : s.shape[1]] = s
        top = jnp.max(s, axis=1, keepdims=True)
        peak = top if peak is None else jnp.maximum(peak, top)
    total = None
    rebuilt = None
    for j in range(n_books):
        expo = jnp.exp(score[j, :, : book_refs[j].shape[0]] - peak)
        mass = jnp.sum(expo, axis=1, keepdims=True)
        total = mass if total is None else total + mass
        if rebuild:
            term = lax.dot_general(expo.astype(BF), book_refs[j][...], NN, preferred_element_type=F32)
            rebuilt = term if rebuilt is None else rebuilt + term
    level = peak + jnp.log(total)
    if not rebuild:
        weight_ref, out_ref = outs
        frames = level.shape[0]
        out_ref[:, :frames] = as_row(level)
        out_ref[:, frames:] = weight_ref[...]
        return
    width = rebuilt.shape[1]
    rebuilt = rebuilt / total
    parts = split(level)
    lane = lax.broadcasted_iota(jnp.int32, (part, EXTRA), 1)
    for j in range(n_rows):
        here = slice(j * part, (j + 1) * part)
        outs[j][:, :width] = rebuilt[here].astype(BF)
        tail = jnp.zeros((part, EXTRA), F32)
        for t in range(n_rows):
            m = (j + t) % n_rows
            for n, value in enumerate(parts):
                tail = jnp.where(lane == 3 * t + n, value[m * part : (m + 1) * part], tail)
        outs[j][:, width:] = tail.astype(BF)


def attend(rows, books, part, weight=None):
    rebuild = weight is None
    more = () if rebuild else (weight,)
    width = books[0].shape[1]
    entries = books[0].shape[0]
    frames = part * len(rows)
    if rebuild:
        out_shape = [jax.ShapeDtypeStruct((part, width + EXTRA), BF)] * len(rows)
    else:
        out_shape = [jax.ShapeDtypeStruct((1, frames + part), F32)]
    total = sum(book.shape[0] for book in books)
    work = 2 * frames * total * width
    return pl.pallas_call(
        functools.partial(attend_kernel, len(rows), len(books), rebuild),
        grid=(1,),
        out_shape=out_shape,
        in_specs=[pl.BlockSpec((part, width), lambda i: (0, 0))] * len(rows)
        + [pl.BlockSpec(book.shape, lambda i: (0, 0)) for book in books + list(more)],
        out_specs=[pl.BlockSpec(s.shape, lambda i: (0, 0)) for s in out_shape],
        scratch_shapes=[
            pltpu.VMEM((frames, width), BF),
            pltpu.VMEM((len(books), frames, entries), F32),
        ],
        compiler_params=pltpu.CompilerParams(vmem_limit_bytes=BYTES),
        cost_estimate=pl.CostEstimate(
            flops=work * (2 if rebuild else 1),
            bytes_accessed=2 * width * (frames + total),
            transcendentals=frames * total,
        ),
        name="attend" if rebuild else "levels",
    )(*rows, *books, *more)


def merge_levels(parts):
    top = functools.reduce(jnp.maximum, parts)
    return top + jnp.log(sum(jnp.exp(part - top) for part in parts))


def combine_kernel(n, *refs):
    frame_ref, piece_refs, (second_ref, level_ref) = refs[0], refs[1 : 1 + n], refs[1 + n :]
    part, width = frame_ref.shape
    tails = [ref[:, width:].astype(F32) for ref in piece_refs]
    for t in reversed(range(n)):
        parts = [tail[:, 3 * t : 3 * t + 1] + tail[:, 3 * t + 1 : 3 * t + 2] + tail[:, 3 * t + 2 : 3 * t + 3] for tail in tails]
        level = merge_levels(parts)
        level_ref[:, t * part : (t + 1) * part] = as_row(level)
    rebuilt = None
    for ref, p in zip(piece_refs, parts):
        term = jnp.exp(p - level) * ref[:, :width].astype(F32)
        rebuilt = term if rebuilt is None else rebuilt + term
    second_ref[...] = (frame_ref[...] - rebuilt).astype(BF)


def combine(frames, pieces):
    part, width = frames.shape
    n = len(pieces)
    return pl.pallas_call(
        functools.partial(combine_kernel, n),
        out_shape=[jax.ShapeDtypeStruct((part, width), BF), jax.ShapeDtypeStruct((1, n * part), F32)],
        in_specs=[pl.BlockSpec(memory_space=pltpu.VMEM)] * (1 + n),
        out_specs=[pl.BlockSpec(memory_space=pltpu.VMEM)] * 2,
        compiler_params=pltpu.CompilerParams(vmem_limit_bytes=BYTES // 4),
        cost_estimate=pl.CostEstimate(flops=4 * part * width * n, bytes_accessed=4 * part * width * n, transcendentals=0),
        name="combine",
    )(frames, *pieces)


def stats_kernel(part, *refs):
    note_refs, out_ref = refs[:-1], refs[-1]
    many = part * len(note_refs)
    turned = []
    for j, ref in enumerate(note_refs):
        row = jnp.broadcast_to(ref[:, :many], (8, many))
        turned.append(pltpu.roll(row, j * part, 1) if j else row)
        out_ref[:, j * part : (j + 1) * part] = ref[:, many:]
    level = merge_levels(turned)[0:1]
    out_ref[...] = jnp.where(out_ref[...] > 0.0, level, FAR)


def stats_of(notes, part):
    return pl.pallas_call(
        functools.partial(stats_kernel, part),
        out_shape=jax.ShapeDtypeStruct((1, part * len(notes)), F32),
        in_specs=[pl.BlockSpec(memory_space=pltpu.VMEM)] * len(notes),
        out_specs=pl.BlockSpec(memory_space=pltpu.VMEM),
        compiler_params=pltpu.CompilerParams(vmem_limit_bytes=BYTES // 8),
        cost_estimate=pl.CostEstimate(flops=100000, bytes_accessed=20000, transcendentals=2000),
        name="stats",
    )(*notes)


def sums_kernel(counts, n_before, refreshed, *refs):
    n_chunks, n_pieces = len(counts), sum(counts)
    piece_refs, rest = refs[:n_pieces], refs[n_pieces:]
    stat_refs, rest = rest[:n_chunks], rest[n_chunks:]
    book_ref, before, rest = rest[0], rest[1 : 1 + n_before], rest[1 + n_before :]
    out_ref, hold = rest[-2:]
    book = book_ref[...]
    width = book.shape[1]
    half = half_column(book)
    num = None
    den = None
    at = 0
    for j, count in enumerate(counts):
        if count == 1:
            chunk = piece_refs[at][...]
        else:
            row_at = 0
            for ref in piece_refs[at : at + count]:
                hold[j % 2, row_at : row_at + ref.shape[0], :] = ref[...]
                row_at += ref.shape[0]
            chunk = hold[j % 2]
        at += count
        s = lax.dot_general(book, chunk, NT, preferred_element_type=F32) - half
        prob = jnp.exp(s - stat_refs[j][...])
        mass = jnp.sum(prob, axis=1, keepdims=True)
        term = lax.dot_general(prob.astype(BF), chunk, NN, preferred_element_type=F32)
        num = term if num is None else num + term
        den = mass if den is None else den + mass
    for ref in before:
        num = num + ref[:, :width]
        den = den + ref[:, width : width + 1]
    if refreshed:
        out_ref[...] = (num + rest[0][...]) / (den + 1.0)
    else:
        out_ref[:, :width] = num
        out_ref[:, width:] = jnp.broadcast_to(den, (den.shape[0], EXTRA))


def sums(chunks, stats, book, before=(), code=None):
    entries, width = book.shape
    pieces = [piece for chunk in chunks for piece in chunk]
    frames = sum(piece.shape[0] for piece in pieces)
    codes = () if code is None else (code,)
    ins = (*pieces, *stats, book, *before, *codes)
    return pl.pallas_call(
        functools.partial(sums_kernel, tuple(len(chunk) for chunk in chunks), len(before), bool(codes)),
        out_shape=jax.ShapeDtypeStruct((entries, width + (0 if codes else EXTRA)), F32),
        in_specs=[pl.BlockSpec(memory_space=pltpu.VMEM)] * len(ins),
        out_specs=pl.BlockSpec(memory_space=pltpu.VMEM),
        scratch_shapes=[pltpu.VMEM((2, stats[0].shape[1], width), BF)],
        compiler_params=pltpu.CompilerParams(vmem_limit_bytes=BYTES),
        cost_estimate=pl.CostEstimate(
            flops=4 * frames * entries * width,
            bytes_accessed=2 * width * frames + 6 * width * entries,
            transcendentals=frames * entries,
        ),
        name="sums",
    )(*ins)


def build(lz, lx, ly, lc):
    entry = ly * lc
    axes = ("dp", "entry")
    sizes = (lz, lx, ly, lc)

    def shift(value, z=0, x=0, y=0, c=0):
        pairs = []
        for source in range(lz * lx * entry):
            rest, place = source, []
            for size in reversed(sizes):
                rest, digit = divmod(rest, size)
                place.append(digit)
            to = 0
            for digit, size, step in zip(reversed(place), sizes, (z, x, y, c)):
                to = to * size + (digit + step) % size
            pairs.append((source, to))
        return lax.ppermute(value, axes, pairs)

    far = [(i, k) for i in range(lx) for k in range(ly)][1:]

    def spread(value):
        return [shift(value, x=i, y=k) for i, k in far]

    straight = [(i, k) for i, k in far if i == 0 or k == 0]
    bent = [(i, k) for i, k in far if i and k]

    def layer(book):
        near = [shift(book, c=m) for m in range(1, lc)]
        got = {(i, k): shift(book, x=i, y=k) for i, k in straight}
        cut = book.shape[0] // 2
        handed = []
        for i, k in bent:
            handed.append(shift(got[0, k][:cut], x=i))
            handed.append(shift(got[i, 0][cut:], y=k))
        pieces = list(got.values())
        across = [shift(p, c=m) for p in pieces for m in range(1, lc)]
        around = [shift(p, c=m) for p in handed for m in range(1, lc)]
        return [book] + near, pieces + handed + across + around

    def on_device(frames, depth, code_one, code_two):
        place = lax.axis_index("entry")
        y, c = place // lc, place % lc
        part = frames.shape[0] // entry
        book_one = code_one.astype(BF)
        book_two = code_two.astype(BF)
        near_one, far_one = layer(book_one)
        starts = [(c * ly + (y - k) % ly) * part for k in range(ly)]
        rows = [lax.dynamic_slice_in_dim(frames, s, part, 0) for s in starts]
        own = rows[0].astype(BF)
        slabs = [own] + [shift(own, z=j) for j in range(1, lz)]
        other = jnp.concatenate(rows[1:], 0).astype(BF) if ly > 1 else own[:0]
        others = [other] + [shift(other, z=j) for j in range(1, lz)] if ly > 1 else []
        pieces = attend(slabs, near_one + far_one, part)
        returned = [pieces[0]] + [shift(pieces[j], z=-j) for j in range(1, lz)]
        near_two, far_two = layer(book_two)

        first = jnp.concatenate(slabs, 0)
        cut = first.shape[0] // 2
        mine = [[piece[(k - 1) * part : k * part] for piece in others] for k in range(1, ly)]
        halves = [jnp.concatenate(m[: len(m) // 2], 0) for m in mine]
        chunks_one = [[first]] + [list(m) for m in mine]
        for i in range(1, lx):
            moved = shift(first, x=i)
            chunks_one.append([moved])
            for k in range(1, ly):
                chunks_one.append([shift(halves[k - 1], x=i), shift(moved[cut:], y=k)])

        group = frames.shape[0] // depth.shape[0]
        if depth.shape[0] == 1:
            weight = jnp.broadcast_to((depth == 2).astype(F32)[:, None], (1, part))
        else:
            weight = jnp.repeat((depth == 2).astype(F32), group)
            weight = lax.dynamic_slice_in_dim(weight, starts[0], part, 0).reshape(1, part)
        second, level = combine(rows[0], returned)

        seconds = [second] + [shift(second, z=j) for j in range(1, lz)]
        ahead = spread(second)
        stats = [level] + spread(level)
        rest = spread(jnp.concatenate(seconds[1:], 0))
        chunks_two = [seconds] + [list(chunk) for chunk in zip(ahead, rest)]
        (note,) = attend(seconds, near_two + far_two, part, weight)
        notes = [note] + [shift(note, z=j) for j in range(1, lz)]

        others = [sums(chunks_one, stats, near_one[m]) for m in range(1, lc)]
        sent = [shift(other, c=-m) for m, other in enumerate(others, 1)]
        new_one = sums(chunks_one, stats, near_one[0], sent, code_one)

        stats = stats_of(notes, part)
        stats = [stats] + spread(stats)
        early = [sums(chunks_two[:-1], stats[:-1], near_two[m]) for m in range(lc)]
        sent = [shift(other, c=-m) for m, other in enumerate(early[1:], 1)]
        last = [chunks_two[-1][0], chunks_two[-1][1]]
        last = [last] + [[shift(last[0], c=m), shift(last[1], c=m)] for m in range(1, lc)]
        stats = [stats[-1]] + [shift(stats[-1], c=m) for m in range(1, lc)]
        new_two = sums(last, stats, near_two[0], [early[0]] + sent, code_two)
        return new_one, new_two

    return on_device


def solution(mesh):
    dp, entry = mesh.shape["dp"], mesh.shape["entry"]
    lz = math.gcd(dp, entry)
    lc = 2 if entry % 2 == 0 else 1
    lx, ly = dp // lz, entry // lc
    return jax.shard_map(
        build(lz, lx, ly, lc),
        mesh=mesh,
        in_specs=(P("dp", None), P("dp"), P(("entry", "dp"), None), P(("entry", "dp"), None)),
        out_specs=(P(("entry", "dp"), None), P(("entry", "dp"), None)),
        check_vma=False,
    )
```

```python
import functools
import math

import jax
import jax.numpy as jnp
from jax import lax
from jax.experimental import pallas as pl
from jax.experimental.pallas import tpu as pltpu
from jax.sharding import PartitionSpec as P


EXTRA = 128
BYTES = 28 * 1024 * 1024
FAR = 3.0e38
NT = (((1,), (1,)), ((), ()))
NN = (((1,), (0,)), ((), ()))
BF = jnp.bfloat16
F32 = jnp.float32


def as_row(column):
    return jnp.broadcast_to(column, (column.shape[0], EXTRA)).T[0:1, :]


def half_column(book):
    wide = book.astype(F32)
    return 0.5 * jnp.sum(wide * wide, axis=1, keepdims=True)


def split(value):
    high = value.astype(BF).astype(F32)
    rest = value - high
    middle = rest.astype(BF).astype(F32)
    return high, middle, rest - middle


def in_lanes(levels):
    lane = lax.broadcasted_iota(jnp.int32, levels[0][0].shape, 1)
    tail = jnp.zeros(levels[0][0].shape, F32)
    for t, parts in enumerate(levels):
        for n, part in enumerate(parts):
            tail = jnp.where(lane == 3 * t + n, part, tail)
    return tail.astype(BF)


def attend_kernel(n_rows, n_books, rebuild, *refs):
    row_refs, book_refs = refs[:n_rows], refs[n_rows : n_rows + n_books]
    outs, (rows, score, joint) = refs[n_rows + n_books : -3], refs[-3:]
    part = row_refs[0].shape[0]
    for j in range(n_rows):
        rows[j * part : (j + 1) * part, :] = row_refs[j][...]
    groups = [[]]
    for ref in book_refs:
        if sum(r.shape[0] for r in groups[-1]) + ref.shape[0] > joint.shape[1]:
            groups.append([])
        groups[-1].append(ref)
    blocks = []
    for n, group in enumerate(groups):
        at = 0
        if len(group) > 1:
            for ref in group:
                joint[n, at : at + ref.shape[0], :] = ref[...]
                at += ref.shape[0]
        blocks.append((group[0], None) if len(group) == 1 else (joint, (n, at)))

    def block(j):
        ref, where = blocks[j]
        return ref[...] if where is None else ref[where[0], : where[1], :]

    sizes = [sum(r.shape[0] for r in group) for group in groups]
    peak = None
    for j in range(len(blocks)):
        book = block(j)
        s = lax.dot_general(rows[...], book, NT, preferred_element_type=F32)
        s = s - as_row(half_column(book))
        score[j, :, : s.shape[1]] = s
        top = jnp.max(s, axis=1, keepdims=True)
        peak = top if peak is None else jnp.maximum(peak, top)
    total = None
    rebuilt = None
    for j in range(len(blocks)):
        expo = jnp.exp(score[j, :, : sizes[j]] - peak)
        mass = jnp.sum(expo, axis=1, keepdims=True)
        total = mass if total is None else total + mass
        if rebuild:
            term = lax.dot_general(expo.astype(BF), block(j), NN, preferred_element_type=F32)
            rebuilt = term if rebuilt is None else rebuilt + term
    level = peak + jnp.log(total)
    if not rebuild:
        weight_ref, out_ref = outs
        frames = level.shape[0]
        out_ref[:, :frames] = as_row(level)
        out_ref[:, frames:] = weight_ref[...]
        return
    width = rebuilt.shape[1]
    rebuilt = rebuilt / total
    parts = split(jnp.broadcast_to(level, (level.shape[0], EXTRA)))
    for j in range(n_rows):
        here = slice(j * part, (j + 1) * part)
        outs[j][:, :width] = rebuilt[here].astype(BF)
        turned = [(j + t) % n_rows for t in range(n_rows)]
        outs[j][:, width:] = in_lanes([[p[m * part : (m + 1) * part] for p in parts] for m in turned])


def attend(rows, books, part, weight=None):
    rebuild = weight is None
    more = () if rebuild else (weight,)
    width = books[0].shape[1]
    entries = books[0].shape[0]
    frames = part * len(rows)
    if rebuild:
        out_shape = [jax.ShapeDtypeStruct((part, width + EXTRA), BF)] * len(rows)
    else:
        out_shape = [jax.ShapeDtypeStruct((1, frames + part), F32)]
    total = sum(book.shape[0] for book in books)
    work = 2 * frames * total * width
    return pl.pallas_call(
        functools.partial(attend_kernel, len(rows), len(books), rebuild),
        grid=(1,),
        out_shape=out_shape,
        in_specs=[pl.BlockSpec((part, width), lambda i: (0, 0))] * len(rows)
        + [pl.BlockSpec(book.shape, lambda i: (0, 0)) for book in books + list(more)],
        out_specs=[pl.BlockSpec(s.shape, lambda i: (0, 0)) for s in out_shape],
        scratch_shapes=[
            pltpu.VMEM((frames, width), BF),
            pltpu.VMEM((len(books), frames, entries), F32),
            pltpu.VMEM((len(books), entries, width), BF),
        ],
        compiler_params=pltpu.CompilerParams(vmem_limit_bytes=BYTES),
        cost_estimate=pl.CostEstimate(
            flops=work * (2 if rebuild else 1),
            bytes_accessed=2 * width * (frames + total),
            transcendentals=frames * total,
        ),
        name="attend" if rebuild else "levels",
    )(*rows, *books, *more)


def merge_levels(parts):
    top = functools.reduce(jnp.maximum, parts)
    return top + jnp.log(sum(jnp.exp(part - top) for part in parts))


def combine_kernel(n, *refs):
    frame_ref, piece_refs, (second_ref, ahead_ref, level_ref) = refs[0], refs[1 : 1 + n], refs[1 + n :]
    part, width = frame_ref.shape
    tails = [ref[:, width:].astype(F32) for ref in piece_refs]
    found = []
    for t in reversed(range(n)):
        parts = [tail[:, 3 * t : 3 * t + 1] + tail[:, 3 * t + 1 : 3 * t + 2] + tail[:, 3 * t + 2 : 3 * t + 3] for tail in tails]
        level = merge_levels(parts)
        level_ref[:, t * part : (t + 1) * part] = as_row(level)
        found.insert(0, split(jnp.broadcast_to(level, (part, EXTRA))))
    rebuilt = None
    for ref, p in zip(piece_refs, parts):
        term = jnp.exp(p - level) * ref[:, :width].astype(F32)
        rebuilt = term if rebuilt is None else rebuilt + term
    second = (frame_ref[...] - rebuilt).astype(BF)
    second_ref[...] = second
    ahead_ref[:, :width] = second
    ahead_ref[:, width:] = in_lanes(found)


def combine(frames, pieces):
    part, width = frames.shape
    n = len(pieces)
    return pl.pallas_call(
        functools.partial(combine_kernel, n),
        out_shape=[
            jax.ShapeDtypeStruct((part, width), BF),
            jax.ShapeDtypeStruct((part, width + EXTRA), BF),
            jax.ShapeDtypeStruct((1, n * part), F32),
        ],
        in_specs=[pl.BlockSpec(memory_space=pltpu.VMEM)] * (1 + n),
        out_specs=[pl.BlockSpec(memory_space=pltpu.VMEM)] * 3,
        compiler_params=pltpu.CompilerParams(vmem_limit_bytes=BYTES // 4),
        cost_estimate=pl.CostEstimate(flops=4 * part * width * n, bytes_accessed=4 * part * width * n, transcendentals=0),
        name="combine",
    )(frames, *pieces)


def stats_kernel(part, *refs):
    note_refs, out_ref = refs[:-1], refs[-1]
    many = part * len(note_refs)
    turned = []
    for j, ref in enumerate(note_refs):
        row = jnp.broadcast_to(ref[:, :many], (8, many))
        turned.append(pltpu.roll(row, j * part, 1) if j else row)
        out_ref[:, j * part : (j + 1) * part] = ref[:, many:]
    level = merge_levels(turned)[0:1]
    out_ref[...] = jnp.where(out_ref[...] > 0.0, level, FAR)


def stats_of(notes, part):
    return pl.pallas_call(
        functools.partial(stats_kernel, part),
        out_shape=jax.ShapeDtypeStruct((1, part * len(notes)), F32),
        in_specs=[pl.BlockSpec(memory_space=pltpu.VMEM)] * len(notes),
        out_specs=pl.BlockSpec(memory_space=pltpu.VMEM),
        compiler_params=pltpu.CompilerParams(vmem_limit_bytes=BYTES // 8),
        cost_estimate=pl.CostEstimate(flops=100000, bytes_accessed=20000, transcendentals=2000),
        name="stats",
    )(*notes)


def sums_kernel(counts, n_before, refreshed, *refs):
    n_chunks, n_pieces = len(counts), sum(counts)
    piece_refs, rest = refs[:n_pieces], refs[n_pieces:]
    stat_refs, rest = rest[:n_chunks], rest[n_chunks:]
    book_ref, before, rest = rest[0], rest[1 : 1 + n_before], rest[1 + n_before :]
    out_ref, hold, row = rest[-3:]
    book = book_ref[...]
    width = book.shape[1]
    half = half_column(book)
    num = None
    den = None
    at = 0
    for j, count in enumerate(counts):
        if count == 1:
            chunk = piece_refs[at][...]
        else:
            row_at = 0
            for ref in piece_refs[at : at + count]:
                hold[j % 2, row_at : row_at + ref.shape[0], :] = ref[:, :width]
                row_at += ref.shape[0]
            chunk = hold[j % 2]
        at += count
        s = lax.dot_general(book, chunk, NT, preferred_element_type=F32) - half
        stat = stat_refs[j]
        if stat.shape[0] == 1:
            level = stat[...]
        else:
            part = stat.shape[0]
            turned = stat[:, width:].astype(F32).T
            for t in range(row.shape[1] // part):
                row[j % 8 : j % 8 + 1, t * part : (t + 1) * part] = sum(turned[3 * t + n : 3 * t + n + 1] for n in (1, 2)) + turned[3 * t : 3 * t + 1]
            level = row[j % 8 : j % 8 + 1, :]
        prob = jnp.exp(s - level)
        mass = jnp.sum(prob, axis=1, keepdims=True)
        term = lax.dot_general(prob.astype(BF), chunk, NN, preferred_element_type=F32)
        num = term if num is None else num + term
        den = mass if den is None else den + mass
    for ref in before:
        num = num + ref[:, :width]
        den = den + ref[:, width : width + 1]
    if refreshed:
        out_ref[...] = (num + rest[0][...]) / (den + 1.0)
    else:
        out_ref[:, :width] = num
        out_ref[:, width:] = jnp.broadcast_to(den, (den.shape[0], EXTRA))


def sums(chunks, stats, book, before=(), code=None):
    entries, width = book.shape
    pieces = [piece for chunk in chunks for piece in chunk]
    frames = sum(piece.shape[0] for piece in pieces)
    codes = () if code is None else (code,)
    many = sum(piece.shape[0] for piece in chunks[0])
    ins = (*pieces, *stats, book, *before, *codes)
    return pl.pallas_call(
        functools.partial(sums_kernel, tuple(len(chunk) for chunk in chunks), len(before), bool(codes)),
        out_shape=jax.ShapeDtypeStruct((entries, width + (0 if codes else EXTRA)), F32),
        in_specs=[pl.BlockSpec(memory_space=pltpu.VMEM)] * len(ins),
        out_specs=pl.BlockSpec(memory_space=pltpu.VMEM),
        scratch_shapes=[pltpu.VMEM((2, many, width), BF), pltpu.VMEM((8, many), F32)],
        compiler_params=pltpu.CompilerParams(vmem_limit_bytes=BYTES),
        cost_estimate=pl.CostEstimate(
            flops=4 * frames * entries * width,
            bytes_accessed=2 * width * frames + 6 * width * entries,
            transcendentals=frames * entries,
        ),
        name="sums",
    )(*ins)


def build(lz, lx, ly, lc):
    entry = ly * lc
    axes = ("dp", "entry")
    sizes = (lz, lx, ly, lc)

    def shift(value, z=0, x=0, y=0, c=0):
        pairs = []
        for source in range(lz * lx * entry):
            rest, place = source, []
            for size in reversed(sizes):
                rest, digit = divmod(rest, size)
                place.append(digit)
            to = 0
            for digit, size, step in zip(reversed(place), sizes, (z, x, y, c)):
                to = to * size + (digit + step) % size
            pairs.append((source, to))
        return lax.ppermute(value, axes, pairs)

    far = [(i, k) for i in range(lx) for k in range(ly)][1:]

    def spread(value):
        return [shift(value, x=i, y=k) for i, k in far]

    straight = [(i, k) for i, k in far if i == 0 or k == 0]
    bent = [(i, k) for i, k in far if i and k]

    def layer(book):
        near = [shift(book, c=m) for m in range(1, lc)]
        got = {(i, k): shift(book, x=i, y=k) for i, k in straight}
        cut = book.shape[0] // 2
        handed = []
        for i, k in bent:
            handed.append(shift(got[0, k][:cut], x=i))
            handed.append(shift(got[i, 0][cut:], y=k))
        pieces = list(got.values())
        across = [shift(p, c=m) for p in pieces for m in range(1, lc)]
        around = [shift(p, c=m) for p in handed for m in range(1, lc)]
        return [book] + near, pieces + handed + across + around

    def on_device(frames, depth, code_one, code_two):
        place = lax.axis_index("entry")
        y, c = place // lc, place % lc
        part = frames.shape[0] // entry
        book_one = code_one.astype(BF)
        book_two = code_two.astype(BF)
        near_one, far_one = layer(book_one)
        starts = [(c * ly + (y - k) % ly) * part for k in range(ly)]
        rows = [lax.dynamic_slice_in_dim(frames, s, part, 0) for s in starts]
        own = rows[0].astype(BF)
        slabs = [own] + [shift(own, z=j) for j in range(1, lz)]
        other = jnp.concatenate(rows[1:], 0).astype(BF) if ly > 1 else own[:0]
        others = [other] + [shift(other, z=j) for j in range(1, lz)] if ly > 1 else []
        pieces = attend(slabs, near_one + far_one, part)
        returned = [pieces[0]] + [shift(pieces[j], z=-j) for j in range(1, lz)]
        near_two, far_two = layer(book_two)

        first = jnp.concatenate(slabs, 0)
        cut = first.shape[0] // 2
        mine = [[piece[(k - 1) * part : k * part] for piece in others] for k in range(1, ly)]
        halves = [jnp.concatenate(m[: len(m) // 2], 0) for m in mine]
        chunks_one = [[first]] + [list(m) for m in mine]
        for i in range(1, lx):
            moved = shift(first, x=i)
            chunks_one.append([moved])
            for k in range(1, ly):
                chunks_one.append([shift(halves[k - 1], x=i), shift(moved[cut:], y=k)])

        group = frames.shape[0] // depth.shape[0]
        if depth.shape[0] == 1:
            weight = jnp.broadcast_to((depth == 2).astype(F32)[:, None], (1, part))
        else:
            weight = jnp.repeat((depth == 2).astype(F32), group)
            weight = lax.dynamic_slice_in_dim(weight, starts[0], part, 0).reshape(1, part)
        second, message, level = combine(rows[0], returned)

        seconds = [second] + [shift(second, z=j) for j in range(1, lz)]
        ahead = spread(message)
        stats = [level] + ahead
        rest = spread(jnp.concatenate(seconds[1:], 0))
        chunks_two = [seconds] + [list(chunk) for chunk in zip(ahead, rest)]
        (note,) = attend(seconds, near_two + far_two, part, weight)
        notes = [note] + [shift(note, z=j) for j in range(1, lz)]

        others = [sums(chunks_one, stats, near_one[m]) for m in range(1, lc)]
        sent = [shift(other, c=-m) for m, other in enumerate(others, 1)]
        new_one = sums(chunks_one, stats, near_one[0], sent, code_one)

        stats = stats_of(notes, part)
        stats = [stats] + spread(stats)
        others = [sums(chunks_two[:-1], stats[:-1], near_two[m]) for m in range(1, lc)]
        sent = [shift(other, c=-m) for m, other in enumerate(others, 1)]
        early = sums(chunks_two[:-1], stats[:-1], near_two[0])
        last = [chunks_two[-1][0], chunks_two[-1][1]]
        last = [last] + [[shift(last[0], c=m), shift(last[1], c=m)] for m in range(1, lc)]
        stats = [stats[-1]] + [shift(stats[-1], c=m) for m in range(1, lc)]
        new_two = sums(last, stats, near_two[0], [early] + sent, code_two)
        return new_one, new_two

    return on_device


def solution(mesh):
    dp, entry = mesh.shape["dp"], mesh.shape["entry"]
    lz = math.gcd(dp, entry)
    lc = 2 if entry % 2 == 0 else 1
    lx, ly = dp // lz, entry // lc
    return jax.shard_map(
        build(lz, lx, ly, lc),
        mesh=mesh,
        in_specs=(P("dp", None), P("dp"), P(("entry", "dp"), None), P(("entry", "dp"), None)),
        out_specs=(P(("entry", "dp"), None), P(("entry", "dp"), None)),
        check_vma=False,
    )
```

```python
import functools
import math

import jax
import jax.numpy as jnp
from jax import lax
from jax.experimental import pallas as pl
from jax.experimental.pallas import tpu as pltpu
from jax.sharding import PartitionSpec as P


EXTRA = 128
BYTES = 28 * 1024 * 1024
FAR = 3.0e38
NT = (((1,), (1,)), ((), ()))
NN = (((1,), (0,)), ((), ()))
BF = jnp.bfloat16
F32 = jnp.float32


def as_row(column):
    return jnp.broadcast_to(column, (column.shape[0], EXTRA)).T[0:1, :]


def half_column(book):
    wide = book.astype(F32)
    return 0.5 * jnp.sum(wide * wide, axis=1, keepdims=True)


def split(value):
    high = value.astype(BF).astype(F32)
    rest = value - high
    middle = rest.astype(BF).astype(F32)
    return high, middle, rest - middle


def in_lanes(levels):
    lane = lax.broadcasted_iota(jnp.int32, levels[0][0].shape, 1)
    tail = jnp.zeros(levels[0][0].shape, F32)
    for t, parts in enumerate(levels):
        for n, part in enumerate(parts):
            tail = jnp.where(lane == 3 * t + n, part, tail)
    return tail.astype(BF)


def attend_kernel(n_rows, n_books, rebuild, *refs):
    row_refs, book_refs = refs[:n_rows], refs[n_rows : n_rows + n_books]
    outs, (rows, score, joint) = refs[n_rows + n_books : -3], refs[-3:]
    part = row_refs[0].shape[0]
    for j in range(n_rows):
        rows[j * part : (j + 1) * part, :] = row_refs[j][...]
    groups = [[]]
    for ref in book_refs:
        if sum(r.shape[0] for r in groups[-1]) + ref.shape[0] > joint.shape[1]:
            groups.append([])
        groups[-1].append(ref)
    blocks = []
    for n, group in enumerate(groups):
        at = 0
        if len(group) > 1:
            for ref in group:
                joint[n, at : at + ref.shape[0], :] = ref[...]
                at += ref.shape[0]
        blocks.append((group[0], None) if len(group) == 1 else (joint, (n, at)))

    def block(j):
        ref, where = blocks[j]
        return ref[...] if where is None else ref[where[0], : where[1], :]

    sizes = [sum(r.shape[0] for r in group) for group in groups]
    peak = None
    for j in range(len(blocks)):
        book = block(j)
        s = lax.dot_general(rows[...], book, NT, preferred_element_type=F32)
        s = s - as_row(half_column(book))
        score[j, :, : s.shape[1]] = s
        top = jnp.max(s, axis=1, keepdims=True)
        peak = top if peak is None else jnp.maximum(peak, top)
    total = None
    rebuilt = None
    for j in range(len(blocks)):
        expo = jnp.exp(score[j, :, : sizes[j]] - peak)
        mass = jnp.sum(expo, axis=1, keepdims=True)
        total = mass if total is None else total + mass
        if rebuild:
            term = lax.dot_general(expo.astype(BF), block(j), NN, preferred_element_type=F32)
            rebuilt = term if rebuilt is None else rebuilt + term
    level = peak + jnp.log(total)
    if not rebuild:
        weight_ref, out_ref = outs
        frames = level.shape[0]
        out_ref[:, :frames] = as_row(level)
        out_ref[:, frames:] = weight_ref[...]
        return
    width = rebuilt.shape[1]
    rebuilt = rebuilt / total
    parts = split(jnp.broadcast_to(level, (level.shape[0], EXTRA)))
    for j in range(n_rows):
        here = slice(j * part, (j + 1) * part)
        outs[j][:, :width] = rebuilt[here].astype(BF)
        turned = [(j + t) % n_rows for t in range(n_rows)]
        outs[j][:, width:] = in_lanes([[p[m * part : (m + 1) * part] for p in parts] for m in turned])


def attend(rows, books, part, weight=None):
    rebuild = weight is None
    more = () if rebuild else (weight,)
    width = books[0].shape[1]
    entries = books[0].shape[0]
    frames = part * len(rows)
    if rebuild:
        out_shape = [jax.ShapeDtypeStruct((part, width + EXTRA), BF)] * len(rows)
    else:
        out_shape = [jax.ShapeDtypeStruct((1, frames + part), F32)]
    total = sum(book.shape[0] for book in books)
    work = 2 * frames * total * width
    return pl.pallas_call(
        functools.partial(attend_kernel, len(rows), len(books), rebuild),
        grid=(1,),
        out_shape=out_shape,
        in_specs=[pl.BlockSpec((part, width), lambda i: (0, 0))] * len(rows)
        + [pl.BlockSpec(book.shape, lambda i: (0, 0)) for book in books + list(more)],
        out_specs=[pl.BlockSpec(s.shape, lambda i: (0, 0)) for s in out_shape],
        scratch_shapes=[
            pltpu.VMEM((frames, width), BF),
            pltpu.VMEM((len(books), frames, entries), F32),
            pltpu.VMEM((len(books), entries, width), BF),
        ],
        compiler_params=pltpu.CompilerParams(vmem_limit_bytes=BYTES),
        cost_estimate=pl.CostEstimate(
            flops=work * (2 if rebuild else 1),
            bytes_accessed=2 * width * (frames + total),
            transcendentals=frames * total,
        ),
        name="attend" if rebuild else "levels",
    )(*rows, *books, *more)


def merge_levels(parts):
    top = functools.reduce(jnp.maximum, parts)
    return top + jnp.log(sum(jnp.exp(part - top) for part in parts))


def combine_kernel(n, *refs):
    frame_ref, piece_refs, (second_ref, ahead_ref, level_ref) = refs[0], refs[1 : 1 + n], refs[1 + n :]
    part, width = frame_ref.shape
    tails = [ref[:, width:].astype(F32) for ref in piece_refs]
    found = []
    for t in reversed(range(n)):
        parts = [tail[:, 3 * t : 3 * t + 1] + tail[:, 3 * t + 1 : 3 * t + 2] + tail[:, 3 * t + 2 : 3 * t + 3] for tail in tails]
        level = merge_levels(parts)
        level_ref[:, t * part : (t + 1) * part] = as_row(level)
        found.insert(0, split(jnp.broadcast_to(level, (part, EXTRA))))
    rebuilt = None
    for ref, p in zip(piece_refs, parts):
        term = jnp.exp(p - level) * ref[:, :width].astype(F32)
        rebuilt = term if rebuilt is None else rebuilt + term
    second = (frame_ref[...] - rebuilt).astype(BF)
    second_ref[...] = second
    ahead_ref[:, :width] = second
    ahead_ref[:, width:] = in_lanes(found)


def combine(frames, pieces):
    part, width = frames.shape
    n = len(pieces)
    return pl.pallas_call(
        functools.partial(combine_kernel, n),
        out_shape=[
            jax.ShapeDtypeStruct((part, width), BF),
            jax.ShapeDtypeStruct((part, width + EXTRA), BF),
            jax.ShapeDtypeStruct((1, n * part), F32),
        ],
        in_specs=[pl.BlockSpec(memory_space=pltpu.VMEM)] * (1 + n),
        out_specs=[pl.BlockSpec(memory_space=pltpu.VMEM)] * 3,
        compiler_params=pltpu.CompilerParams(vmem_limit_bytes=BYTES // 4),
        cost_estimate=pl.CostEstimate(flops=4 * part * width * n, bytes_accessed=4 * part * width * n, transcendentals=0),
        name="combine",
    )(frames, *pieces)


def stats_kernel(part, *refs):
    note_refs, out_ref = refs[:-1], refs[-1]
    many = part * len(note_refs)
    turned = []
    for j, ref in enumerate(note_refs):
        row = jnp.broadcast_to(ref[:, :many], (8, many))
        turned.append(pltpu.roll(row, j * part, 1) if j else row)
        out_ref[:, j * part : (j + 1) * part] = ref[:, many:]
    level = merge_levels(turned)[0:1]
    out_ref[...] = jnp.where(out_ref[...] > 0.0, level, FAR)


def stats_of(notes, part):
    return pl.pallas_call(
        functools.partial(stats_kernel, part),
        out_shape=jax.ShapeDtypeStruct((1, part * len(notes)), F32),
        in_specs=[pl.BlockSpec(memory_space=pltpu.VMEM)] * len(notes),
        out_specs=pl.BlockSpec(memory_space=pltpu.VMEM),
        compiler_params=pltpu.CompilerParams(vmem_limit_bytes=BYTES // 8),
        cost_estimate=pl.CostEstimate(flops=100000, bytes_accessed=20000, transcendentals=2000),
        name="stats",
    )(*notes)


def sums_kernel(counts, n_before, refreshed, *refs):
    n_chunks, n_pieces = len(counts), sum(counts)
    piece_refs, rest = refs[:n_pieces], refs[n_pieces:]
    stat_refs, rest = rest[:n_chunks], rest[n_chunks:]
    book_ref, before, rest = rest[0], rest[1 : 1 + n_before], rest[1 + n_before :]
    out_ref, hold, row = rest[-3:]
    book = book_ref[...]
    width = book.shape[1]
    half = half_column(book)
    num = None
    den = None
    at = 0
    for j, count in enumerate(counts):
        if count == 1:
            chunk = piece_refs[at][...]
        else:
            row_at = 0
            for ref in piece_refs[at : at + count]:
                hold[j % 2, row_at : row_at + ref.shape[0], :] = ref[:, :width]
                row_at += ref.shape[0]
            chunk = hold[j % 2]
        at += count
        s = lax.dot_general(book, chunk, NT, preferred_element_type=F32) - half
        stat = stat_refs[j]
        if stat.shape[0] == 1:
            level = stat[...]
        else:
            part = stat.shape[0]
            turned = stat[:, width:].astype(F32).T
            for t in range(row.shape[1] // part):
                row[j % 8 : j % 8 + 1, t * part : (t + 1) * part] = sum(turned[3 * t + n : 3 * t + n + 1] for n in (1, 2)) + turned[3 * t : 3 * t + 1]
            level = row[j % 8 : j % 8 + 1, :]
        prob = jnp.exp(s - level)
        mass = jnp.sum(prob, axis=1, keepdims=True)
        term = lax.dot_general(prob.astype(BF), chunk, NN, preferred_element_type=F32)
        num = term if num is None else num + term
        den = mass if den is None else den + mass
    for ref in before:
        num = num + ref[:, :width]
        den = den + ref[:, width : width + 1]
    if refreshed:
        out_ref[...] = (num + rest[0][...]) / (den + 1.0)
    else:
        out_ref[:, :width] = num
        out_ref[:, width:] = jnp.broadcast_to(den, (den.shape[0], EXTRA))


def sums(chunks, stats, book, before=(), code=None):
    entries, width = book.shape
    pieces = [piece for chunk in chunks for piece in chunk]
    frames = sum(piece.shape[0] for piece in pieces)
    codes = () if code is None else (code,)
    many = sum(piece.shape[0] for piece in chunks[0])
    ins = (*pieces, *stats, book, *before, *codes)
    return pl.pallas_call(
        functools.partial(sums_kernel, tuple(len(chunk) for chunk in chunks), len(before), bool(codes)),
        out_shape=jax.ShapeDtypeStruct((entries, width + (0 if codes else EXTRA)), F32),
        in_specs=[pl.BlockSpec(memory_space=pltpu.VMEM)] * len(ins),
        out_specs=pl.BlockSpec(memory_space=pltpu.VMEM),
        scratch_shapes=[pltpu.VMEM((2, many, width), BF), pltpu.VMEM((8, many), F32)],
        compiler_params=pltpu.CompilerParams(vmem_limit_bytes=BYTES),
        cost_estimate=pl.CostEstimate(
            flops=4 * frames * entries * width,
            bytes_accessed=2 * width * frames + 6 * width * entries,
            transcendentals=frames * entries,
        ),
        name="sums",
    )(*ins)


def build(lz, lx, ly, lc):
    entry = ly * lc
    axes = ("dp", "entry")
    sizes = (lz, lx, ly, lc)

    def shift(value, z=0, x=0, y=0, c=0):
        pairs = []
        for source in range(lz * lx * entry):
            rest, place = source, []
            for size in reversed(sizes):
                rest, digit = divmod(rest, size)
                place.append(digit)
            to = 0
            for digit, size, step in zip(reversed(place), sizes, (z, x, y, c)):
                to = to * size + (digit + step) % size
            pairs.append((source, to))
        return lax.ppermute(value, axes, pairs)

    far = [(i, k) for i in range(lx) for k in range(ly)][1:]

    def spread(value):
        return [shift(value, x=i, y=k) for i, k in far]

    straight = [(i, k) for i, k in far if i == 0 or k == 0]
    bent = [(i, k) for i, k in far if i and k]

    def layer(book):
        near = [shift(book, c=m) for m in range(1, lc)]
        got = {(i, k): shift(book, x=i, y=k) for i, k in straight}
        cut = book.shape[0] // 2
        handed = []
        for i, k in bent:
            handed.append(shift(got[0, k][:cut], x=i))
            handed.append(shift(got[i, 0][cut:], y=k))
        pieces = list(got.values())
        across = [shift(p, c=m) for p in pieces for m in range(1, lc)]
        around = [shift(p, c=m) for p in handed for m in range(1, lc)]
        return [book] + near, pieces + handed + across + around

    def on_device(frames, depth, code_one, code_two):
        place = lax.axis_index("entry")
        y, c = place // lc, place % lc
        part = frames.shape[0] // entry
        book_one = code_one.astype(BF)
        book_two = code_two.astype(BF)
        near_one, far_one = layer(book_one)
        starts = [(c * ly + (y - k) % ly) * part for k in range(ly)]
        rows = [lax.dynamic_slice_in_dim(frames, s, part, 0) for s in starts]
        own = rows[0].astype(BF)
        slabs = [own] + [shift(own, z=j) for j in range(1, lz)]
        other = jnp.concatenate(rows[1:], 0).astype(BF) if ly > 1 else own[:0]
        others = [other] + [shift(other, z=j) for j in range(1, lz)] if ly > 1 else []
        pieces = attend(slabs, near_one + far_one, part)
        returned = [pieces[0]] + [shift(pieces[j], z=-j) for j in range(1, lz)]
        near_two, far_two = layer(book_two)

        first = jnp.concatenate(slabs, 0)
        cut = first.shape[0] // 2
        mine = [[piece[(k - 1) * part : k * part] for piece in others] for k in range(1, ly)]
        halves = [jnp.concatenate(m[: len(m) // 2], 0) for m in mine]
        chunks_one = [[first]] + [list(m) for m in mine]
        for i in range(1, lx):
            moved = shift(first, x=i)
            chunks_one.append([moved])
            for k in range(1, ly):
                chunks_one.append([shift(halves[k - 1], x=i), shift(moved[cut:], y=k)])

        group = frames.shape[0] // depth.shape[0]
        if depth.shape[0] == 1:
            weight = jnp.broadcast_to((depth == 2).astype(F32)[:, None], (1, part))
        else:
            weight = jnp.repeat((depth == 2).astype(F32), group)
            weight = lax.dynamic_slice_in_dim(weight, starts[0], part, 0).reshape(1, part)
        second, message, level = combine(rows[0], returned)

        seconds = [second] + [shift(second, z=j) for j in range(1, lz)]
        ahead = spread(message)
        stats = [level] + ahead
        rest = spread(jnp.concatenate(seconds[1:], 0))
        chunks_two = [seconds] + [list(chunk) for chunk in zip(ahead, rest)]
        (note,) = attend(seconds, near_two + far_two, part, weight)
        notes = [note] + [shift(note, z=j) for j in range(1, lz)]

        others = [sums(chunks_one, stats, near_one[m]) for m in range(1, lc)]
        sent = [shift(other, c=-m) for m, other in enumerate(others, 1)]
        new_one = sums(chunks_one, stats, near_one[0], sent, code_one)

        stats = stats_of(notes, part)
        stats = [stats] + spread(stats)
        begun = [sums(chunks_two[:1], stats[:1], near_two[m]) for m in range(lc)]
        others = [sums(chunks_two[1:-1], stats[1:-1], near_two[m], begun[m : m + 1]) for m in range(1, lc)]
        sent = [shift(other, c=-m) for m, other in enumerate(others, 1)]
        early = sums(chunks_two[1:-1], stats[1:-1], near_two[0], begun[:1])
        last = [chunks_two[-1][0], chunks_two[-1][1]]
        last = [last] + [[shift(last[0], c=m), shift(last[1], c=m)] for m in range(1, lc)]
        stats = [stats[-1]] + [shift(stats[-1], c=m) for m in range(1, lc)]
        new_two = sums(last, stats, near_two[0], [early] + sent, code_two)
        return new_one, new_two

    return on_device


def solution(mesh):
    dp, entry = mesh.shape["dp"], mesh.shape["entry"]
    lz = math.gcd(dp, entry)
    lc = 2 if entry % 2 == 0 else 1
    lx, ly = dp // lz, entry // lc
    return jax.shard_map(
        build(lz, lx, ly, lc),
        mesh=mesh,
        in_specs=(P("dp", None), P("dp"), P(("entry", "dp"), None), P(("entry", "dp"), None)),
        out_specs=(P(("entry", "dp"), None), P(("entry", "dp"), None)),
        check_vma=False,
    )
```
